32 devices in a mesh: member: 2 (over x), gx: 16 (over z, y, core).
Axes of the slice: x: 2, y: 2, z: 4, core: 2. Of those that a mesh axis runs over, the one named last changes fastest.
Arguments:
- spectrum: float32 [36, 32, 256, 128], P(None, None, ('member', 'gx')), parts along dimension 2, may hold values from 0 to 1
- wind: float32 [2, 256, 128], P(None, ('member', 'gx')), parts along dimension 1, may hold values from -32 to 32
- land_sea: int32 [128, 128], P('gx'), may hold values 0 or 1
- band_rows: int32 [128], replicated, may hold values from 0 to 127, each once
Outputs:
- spectrum_next: float32 [36, 32, 256, 128], P(None, None, ('member', 'gx')), parts along dimension 2
- ocean_fields: float32 [4, 128, 256], P(None, 'gx', 'member'), parts along dimension 2
The draws below stay inside these ranges and needn't reach their ends.
There are 2 independent parts, one for each index of `member`. The reference program is written for one: setup_inputs(seed, part) draws one part's arguments, and reference() takes and returns one part's arrays. A program takes and returns all parts, laid end to end along the dimension named above; an argument that names none is the same for every part. Nothing has to cross between parts.
Inputs may be any that keep to these rules, and one draw needn't show every extreme that they name: band_rows names each of the 128 latitude rows exactly once.
All inputs are finite; a program needn't handle non-finite values. No bound on the sum of `land_sea` on one device may be relied on, other than what follows from the above.
Results may differ from the reference program's by a relative error of at most 0.00015.
Values sent between devices are 32-bit elements; how exact they have to be, the bound alone decides.
No kernel may reach another device: no remote copies, remote signals or barrier semaphores. Data moves between devices by JAX's collectives and lax.ppermute only.
A program may use at most 128 MiB of HBM per device.

```python
import math
import jax
import jax.numpy as jnp
from jax import lax

DIRS = 36
FREQS = 32
LAT = 128
STEPS = 3
NLON = 128


def touch_ends(values, key, least, largest):
    index_at = [jax.random.randint(jax.random.fold_in(key, axis), (), 0, length) for axis, length in enumerate(values.shape)]
    longest = values.shape.index(max(values.shape))
    beside = index_at[:longest] + [(index_at[longest] + 1) % values.shape[longest]] + index_at[longest + 1:]
    return values.at[tuple(index_at)].set(least).at[tuple(beside)].set(largest)


def block_levels(own_key, shape, shards, least, largest):
    def one(position, shards_of):
        draws = jax.random.uniform(jax.random.fold_in(jax.random.fold_in(own_key, 6), position), (shards_of,), jnp.float32, least / len(shards), largest / len(shards))
        return jnp.repeat(jnp.exp(draws), shape[position] // shards_of).reshape((-1,) + (1,) * (len(shape) - position - 1))

    loudness = one(*shards[0])
    for cut in shards[1:]:
        loudness = loudness * one(*cut)
    return loudness


def centred(rng, dims, width, bound, cuts=(), kind=jnp.bfloat16):
    level = block_levels(rng, dims, cuts, -0.22, 0.18) if cuts else 1.0
    array = jax.random.normal(rng, dims, jnp.float32) * width * level
    return jnp.minimum(jnp.maximum(array, -bound), bound).astype(kind)


def setup_inputs(seed: int = 0, part: int = 0) -> dict:
    keys = jax.random.split(jax.random.key(seed), 5)
    part_keys = jax.random.split(jax.random.fold_in(keys[4], part), 5)
    spectrum = jnp.clip(1.0 * jax.random.uniform(part_keys[0], (DIRS, FREQS, NLON, LAT), jnp.float32) ** block_levels(part_keys[0], (DIRS, FREQS, NLON, LAT), ((2, 16),), -0.2, 0.2), 0.0, 1.0)
    wind = centred(part_keys[1], (2, NLON, LAT), 8.0, 32.0, ((1, 16),), jnp.float32)
    land_sea = touch_ends((jax.random.randint(keys[2], (NLON, LAT), 0, 4) < 3).astype(jnp.int32), jax.random.fold_in(keys[2], 1), 0, 1)
    band_rows = jax.random.permutation(keys[3], LAT).astype(jnp.int32)
    return dict(spectrum=spectrum, wind=wind, land_sea=land_sea, band_rows=band_rows)


def wave_tables(directions, frequencies):
    angles = (jnp.arange(directions, dtype=jnp.float32) + 0.5) * (2.0 * math.pi / directions)
    levels = jnp.arange(frequencies, dtype=jnp.float32)
    shrink = jnp.power(jnp.float32(1.1), -levels)
    frequency = 0.0418 / shrink
    inverse_speed = 2.0 * math.pi * frequency / 9.81
    weight = (levels + 1.0) / frequencies
    cosine_dir = jnp.cos(angles)[:, None]
    sine_dir = jnp.sin(angles)[:, None]
    courant_x = 0.45 * shrink[None, :] * cosine_dir
    courant_y = 0.45 * shrink[None, :] * sine_dir
    factor = 3.0 / math.sqrt(directions * frequencies)
    project = jnp.stack([factor * weight[None, :] * cosine_dir, factor * weight[None, :] * sine_dir])
    return (courant_x, courant_y, cosine_dir, sine_dir, inverse_speed, weight * weight, project)

def upwind(center, west_cell, east_cell, courant_x, courant_y):
    along_x = courant_x[:, :, None, None]
    along_y = courant_y[:, :, None, None]
    border = jnp.zeros_like(center[..., :1])
    south_cell = jnp.concatenate([border, center[..., :-1]], axis=3)
    north_cell = jnp.concatenate([center[..., 1:], border], axis=3)
    return center - jnp.maximum(along_x, 0.0) * (center - west_cell) + jnp.maximum(-along_x, 0.0) * (east_cell - center) - jnp.maximum(along_y, 0.0) * (center - south_cell) + jnp.maximum(-along_y, 0.0) * (north_cell - center)

def sources(advected, wind_east, wind_north, sea_mask, tables):
    cosine_dir, sine_dir, inverse_speed, weight_two = (tables[2], tables[3], tables[4], tables[5])
    advected = advected * sea_mask
    energy = lax.optimization_barrier(jnp.mean(advected, axis=(0, 1)))
    wind_ratio = (wind_east * cosine_dir[:, :, None, None] + wind_north * sine_dir[:, :, None, None]) * inverse_speed[None, :, None, None]
    growth = 0.05 * jnp.clip(wind_ratio - 1.0, 0.0, 4.0)
    damping = 0.3 * weight_two[None, :, None, None] * (energy / (0.5 + energy))
    return (advected * (1.0 + growth) / (1.0 + damping), growth * advected)

def coupling_fields(input_flux, current, project):
    stress = jnp.einsum('cij,ijxy->cxy', project, input_flux, precision=lax.Precision.HIGHEST)
    stokes = jnp.einsum('cij,ijxy->cxy', project, current, precision=lax.Precision.HIGHEST)
    return jnp.concatenate([stress, stokes], axis=0)

def reference(spectrum, wind, land_sea, band_rows):
    tables = wave_tables(spectrum.shape[0], spectrum.shape[1])
    sea_mask = land_sea.astype(jnp.float32)
    current = spectrum
    for step_index in range(STEPS):
        advected = upwind(current, jnp.roll(current, 1, axis=2), jnp.roll(current, -1, axis=2), tables[0], tables[1])
        current, input_flux = sources(advected, wind[0], wind[1], sea_mask, tables)
    fields = coupling_fields(input_flux, current, tables[6])
    ocean_fields = jnp.transpose(fields[:, :, band_rows], (0, 2, 1))
    return (current, ocean_fields)
```

```python
import math

import jax
import jax.numpy as jnp
from jax import lax
from jax.experimental import pallas as pl
from jax.experimental.pallas import tpu as pltpu
from jax.sharding import PartitionSpec as P

VMEM = pl.BlockSpec(memory_space=pltpu.VMEM)
HBM = pl.BlockSpec(memory_space=pl.ANY)
LIMIT = 48 * 1024 * 1024
F32 = jnp.float32


def passed_along(value, steps):
    count = lax.axis_size("gx")
    pairs = [(source, (source + steps) % count) for source in range(count)]
    return lax.ppermute(value, "gx", pairs)


def shrink(level):
    return 0.45 * 1.1 ** (-level)


def wind_factor(level):
    return 0.05 * 2.0 * math.pi * 0.0418 * 1.1**level / 9.81


def quadrants(directions):
    quarter = directions // 4
    return (
        (0, True, True, 0),
        (quarter, False, True, 0),
        (2 * quarter, False, False, quarter),
        (3 * quarter, True, False, quarter),
    )


def growth_of(ratio, level):
    return jnp.clip(ratio * wind_factor(level) - 0.05, 0.0, 0.2)


def damping_ratio(energy_sum, sea, bins):
    energy = sea * energy_sum * (1.0 / bins)
    return energy / (0.5 + energy)


def directions_loop(directions, start, body, shape, state):
    delta = 2.0 * math.pi / directions
    turn_c, turn_s = math.cos(delta), math.sin(delta)
    first = (start + 0.5) * delta

    def step(place, carry):
        cosine, sine, state = carry
        state = body(place, cosine, sine, state)
        return cosine * turn_c - sine * turn_s, sine * turn_c + cosine * turn_s, state

    begin = (jnp.full(shape, math.cos(first), F32), jnp.full(shape, math.sin(first), F32), state)
    return lax.fori_loop(0, directions // 4, step, begin)[2]


def flow(cosine, sine, eastward, northward):
    shape = cosine.shape
    row = lax.broadcasted_iota(jnp.int32, shape, 0)
    lane = lax.broadcasted_iota(jnp.int32, shape, 1)
    edge_row = 0 if eastward else shape[0] - 1
    edge_lane = 0 if northward else shape[1] - 1
    pace_x, pace_y = jnp.abs(cosine), jnp.abs(sine)
    inner_x = jnp.where(row == edge_row, 0.0, pace_x)
    halo_x = jnp.where(row == edge_row, pace_x, 0.0)
    inner_y = jnp.where(lane == edge_lane, 0.0, pace_y)
    return inner_x, halo_x, inner_y, pace_x + pace_y


def advect(cell, inner_x, inner_y, both, eastward, northward, level):
    rows, lanes = cell.shape
    up_x = pltpu.roll(cell, 1 if eastward else rows - 1, 0)
    up_y = pltpu.roll(cell, 1 if northward else lanes - 1, 1)
    return cell + shrink(level) * (inner_x * up_x + inner_y * up_y - both * cell)


def columns_kernel(spectrum, *outs):
    directions, levels, rows, lanes = spectrum.shape
    quarter = directions // 4
    for start, eastward, _, place in quadrants(directions):
        for depth in range(3):
            out = outs[depth if eastward else 3 + depth]
            column = rows - 1 - depth if eastward else depth

            def move(n, _, out=out, column=column, start=start, place=place):
                flat = spectrum.at[start + n].reshape(levels * rows, lanes)
                out[place + n] = flat[pl.ds(column, levels, stride=rows), :]
                return 0

            lax.fori_loop(0, quarter, move, 0)


def first_kernel(spectrum, advected, energy):
    directions, levels, rows, lanes = spectrum.shape
    total = jnp.zeros((rows, lanes), F32)
    for start, eastward, northward, _ in quadrants(directions):

        def body(n, cosine, sine, total, start=start, eastward=eastward, northward=northward):
            inner_x, _, inner_y, both = flow(cosine, sine, eastward, northward)
            for level in range(levels):
                cell = spectrum[start + n, level]
                moved = advect(cell, inner_x, inner_y, both, eastward, northward, level)
                advected[start + n, level] = moved
                total = total + moved
            return total

        total = directions_loop(directions, start, body, (rows, lanes), total)
    energy[...] = total


def fill_factors(factors, energy, sea, bins, levels):
    ratio = damping_ratio(energy[...], sea[...], bins)
    for level in range(levels):
        weight = (level + 1.0) / levels
        factors[level] = sea[...] / (1.0 + (0.3 * weight * weight) * ratio)


def next_kernel(before, energy_in, wind, sea, from_west, from_east, advected, energy, factors):
    directions, levels, rows, lanes = before.shape
    fill_factors(factors, energy_in, sea, directions * levels, levels)
    total = jnp.zeros((rows, lanes), F32)
    for start, eastward, northward, place in quadrants(directions):
        halo = from_west if eastward else from_east

        def body(n, cosine, sine, total, start=start, eastward=eastward, northward=northward, place=place, halo=halo):
            inner_x, halo_x, inner_y, both = flow(cosine, sine, eastward, northward)
            ratio = wind[0] * cosine + wind[1] * sine
            for level in range(levels):
                edge = jnp.broadcast_to(halo[place + n, pl.ds(level, 1), :], (rows, lanes))
                cell = before[start + n, level] + (shrink(level) * halo_x) * edge
                cell = cell * (1.0 + growth_of(ratio, level)) * factors[level]
                moved = advect(cell, inner_x, inner_y, both, eastward, northward, level)
                advected[start + n, level] = moved
                total = total + moved
            return total

        total = directions_loop(directions, start, body, (rows, lanes), total)
    energy[...] = total


def last_kernel(before, energy_in, wind, sea, from_west, from_east, bands, spectrum, fields, factors, staged, sems):
    directions, levels, rows, lanes = before.shape
    quarter = directions // 4
    fill_factors(factors, energy_in, sea, directions * levels, levels)
    zero = jnp.zeros((rows, lanes), F32)
    sums = (zero, zero, zero, zero)

    def out_copy(index):
        return pltpu.make_async_copy(staged.at[index], spectrum.at[index], sems.at[index])

    for start, eastward, northward, place in quadrants(directions):
        halo = from_west if eastward else from_east

        def body(n, cosine, sine, sums, start=start, eastward=eastward, northward=northward, place=place, halo=halo):
            _, halo_x, _, _ = flow(cosine, sine, eastward, northward)
            ratio = wind[0] * cosine + wind[1] * sine
            input_sum, current_sum = zero, zero
            for level in range(levels):
                weight = (level + 1.0) / levels
                edge = jnp.broadcast_to(halo[place + n, pl.ds(level, 1), :], (rows, lanes))
                moved = before[start + n, level] + (shrink(level) * halo_x) * edge
                growth = growth_of(ratio, level)
                gained = growth * moved
                cell = (moved + gained) * factors[level]
                staged[start + n, level] = cell
                input_sum = input_sum + weight * gained
                current_sum = current_sum + weight * cell
            out_copy(start + n).start()
            return (
                sums[0] + cosine * input_sum,
                sums[1] + sine * input_sum,
                sums[2] + cosine * current_sum,
                sums[3] + sine * current_sum,
            )

        sums = directions_loop(directions, start, body, (rows, lanes), sums)
    scale = 3.0 / math.sqrt(directions * levels)
    mask = sea[...] * scale
    stacked = jnp.concatenate([sums[0] * mask, sums[1] * mask, sums[2] * scale, sums[3] * scale], axis=0)
    wanted = jnp.broadcast_to(bands[...], (lanes, bands.shape[1]))
    choose = (lax.broadcasted_iota(jnp.int32, wanted.shape, 0) == wanted).astype(F32)
    picked = jnp.dot(stacked, choose, precision=lax.Precision.HIGHEST, preferred_element_type=F32)
    fields[...] = picked.T

    def finish(index, _):
        out_copy(index).wait()
        return 0

    lax.fori_loop(0, directions, finish, 0)


def by_level(levels, lanes, function):
    level = lax.broadcasted_iota(jnp.int32, (levels, lanes), 0).astype(F32)
    return function(level)


def side_angles(directions, eastward):
    listed = []
    for start, east, northward, place in quadrants(directions):
        if east == eastward:
            for n in range(directions // 4):
                angle = (start + n + 0.5) * (2.0 * math.pi / directions)
                listed.append((place + n, math.cos(angle), math.sin(angle), northward))
    return listed


def growth_factor(levels, lanes):
    power = by_level(levels, lanes, lambda level: jnp.exp(level * math.log(1.1)))
    return power * wind_factor(0)


def halo_energy(halo, paces, directions, eastward):
    levels, lanes = paces.shape
    total = jnp.zeros((levels, lanes), F32)
    for place, cosine, _, _ in side_angles(directions, eastward):
        total = total + abs(cosine) * halo[place]
    return jnp.sum(total * paces, axis=0, keepdims=True)


def with_halo_energy(partial, west_sum, east_sum):
    row = lax.broadcasted_iota(jnp.int32, partial.shape, 0)
    add = jnp.where(row == 0, west_sum, 0.0) + jnp.where(row == partial.shape[0] - 1, east_sum, 0.0)
    return partial + add


def paces_of(levels, lanes):
    return by_level(levels, lanes, lambda level: 0.45 * jnp.exp(level * -math.log(1.1)))


def pick(array, row):
    return array[row : row + 1, :]


def energy_kernel(partial, wind, sea, from_west, from_east, energy, to_east, to_west):
    half, levels, lanes = from_west.shape
    rows = partial.shape[0]
    paces = paces_of(levels, lanes)
    west_sum = halo_energy(from_west, paces, 2 * half, True)
    east_sum = halo_energy(from_east, paces, 2 * half, False)
    full = with_halo_energy(partial[...], west_sum, east_sum)
    energy[...] = full
    mask, wind_x, wind_y = sea[...], wind[0], wind[1]
    for out, near, far in ((to_east, rows - 1, rows - 2), (to_west, 0, 1)):
        parts = []
        for column in (near, far):
            parts += [pick(full, column), pick(wind_x, column), pick(wind_y, column), pick(mask, column)]
        out[...] = jnp.concatenate(parts, axis=0)


def column_step(near, far, out, facts, directions, eastward, paces, winds):
    levels, lanes = paces.shape
    energy, wind_x, wind_y, mask = facts
    ratio = damping_ratio(energy, mask, directions * levels)
    weight = by_level(levels, lanes, lambda level: (level + 1.0) * (1.0 / levels))
    factor = mask / (1.0 + 0.3 * weight * weight * ratio)
    lane = lax.broadcasted_iota(jnp.int32, (levels, lanes), 1)
    for place, cosine, sine, northward in side_angles(directions, eastward):
        cell = near[place]
        up_y = pltpu.roll(cell, 1 if northward else lanes - 1, 1)
        up_y = jnp.where(lane == (0 if northward else lanes - 1), 0.0, up_y)
        change = abs(cosine) * far[place] + abs(sine) * up_y - (abs(cosine) + abs(sine)) * cell
        moved = cell + paces * change
        growth = jnp.clip((wind_x * cosine + wind_y * sine) * winds - 0.05, 0.0, 0.2)
        out[place] = (moved + growth * moved) * factor


def facts_at(message, depth, energy=None):
    rows = [message[4 * depth + k : 4 * depth + k + 1, :] for k in range(4)]
    if energy is not None:
        rows[0] = energy
    return rows


def second_kernel(partial, west_near, west_far, east_near, east_far, west_facts, east_facts,
                  west_next, east_next, energy, to_east, to_west):
    half, levels, lanes = west_near.shape
    rows = partial.shape[0]
    paces = paces_of(levels, lanes)
    winds = growth_factor(levels, lanes)
    column_step(west_near, west_far, west_next, facts_at(west_facts, 0), 2 * half, True, paces, winds)
    column_step(east_near, east_far, east_next, facts_at(east_facts, 0), 2 * half, False, paces, winds)
    west_sum = halo_energy(west_next, paces, 2 * half, True)
    east_sum = halo_energy(east_next, paces, 2 * half, False)
    full = with_halo_energy(partial[...], west_sum, east_sum)
    energy[...] = full
    to_east[...] = jnp.broadcast_to(pick(full, rows - 1), to_east.shape)
    to_west[...] = jnp.broadcast_to(pick(full, 0), to_west.shape)


def third_kernel(partial, west_near, west_mid, west_far, east_near, east_mid, east_far,
                 west_facts, east_facts, west_energy, east_energy,
                 west_next, east_next, energy, scratch):
    half, levels, lanes = west_near.shape
    paces = paces_of(levels, lanes)
    winds = growth_factor(levels, lanes)
    for near, mid, far, facts, newer, out, eastward in (
        (west_near, west_mid, west_far, west_facts, west_energy, west_next, True),
        (east_near, east_mid, east_far, east_facts, east_energy, east_next, False),
    ):
        column_step(mid, far, scratch, facts_at(facts, 1), 2 * half, eastward, paces, winds)
        later = facts_at(facts, 0, newer[0:1, :])
        column_step(near, scratch, out, later, 2 * half, eastward, paces, winds)
    west_sum = halo_energy(west_next, paces, 2 * half, True)
    east_sum = halo_energy(east_next, paces, 2 * half, False)
    energy[...] = with_halo_energy(partial[...], west_sum, east_sum)


def per_device(spectrum, wind, land_sea, band_rows):
    directions, levels, rows, lanes = spectrum.shape
    half = directions // 2
    sea = land_sea.astype(F32)
    full = jax.ShapeDtypeStruct(spectrum.shape, F32)
    plane = jax.ShapeDtypeStruct((rows, lanes), F32)
    column = jax.ShapeDtypeStruct((half, levels, lanes), F32)
    note = jax.ShapeDtypeStruct((8, lanes), F32)
    params = pltpu.CompilerParams(vmem_limit_bytes=LIMIT)
    factors = pltpu.VMEM((levels, rows, lanes), F32)

    def call(kernel, count, outs, scratch=(), out_specs=None):
        return pl.pallas_call(
            kernel,
            in_specs=[VMEM] * count,
            out_specs=[VMEM] * len(outs) if out_specs is None else out_specs,
            out_shape=outs,
            scratch_shapes=list(scratch),
            compiler_params=params,
            name=kernel.__name__,
        )

    columns = call(columns_kernel, 1, [column] * 6)(spectrum)
    west_1, east_1 = passed_along(columns[0], 1), passed_along(columns[3], -1)
    west_2, east_2 = passed_along(columns[1], 1), passed_along(columns[4], -1)
    moved, partial = call(first_kernel, 1, [full, plane])(spectrum)
    energy, to_east, to_west = call(energy_kernel, 5, [plane, note, note])(
        partial, wind, sea, west_1, east_1
    )
    west_facts, east_facts = passed_along(to_east, 1), passed_along(to_west, -1)
    third_west, third_east, _ = lax.optimization_barrier((columns[2], columns[5], energy))
    west_3, east_3 = passed_along(third_west, 1), passed_along(third_east, -1)
    step = call(next_kernel, 6, [full, plane], [factors])
    moved, partial = step(moved, energy, wind, sea, west_1, east_1)
    west_b, east_b, energy, to_east, to_west = call(
        second_kernel, 7, [column, column, plane, note, note]
    )(partial, west_1, west_2, east_1, east_2, west_facts, east_facts)
    west_energy, east_energy = passed_along(to_east, 1), passed_along(to_west, -1)
    moved, partial = step(moved, energy, wind, sea, west_b, east_b)
    west_c, east_c, energy = call(
        third_kernel, 11, [column, column, plane], [pltpu.VMEM((half, levels, lanes), F32)]
    )(partial, west_b, west_2, west_3, east_b, east_2, east_3, west_facts, east_facts, west_energy, east_energy)
    return finish(moved, energy, wind, sea, west_c, east_c, band_rows, call, full, factors)


def finish(moved, energy, wind, sea, west, east, band_rows, call, full, factors):
    directions, levels, rows, lanes = moved.shape
    bands = band_rows.shape[0]
    spectrum_next, local = call(
        last_kernel,
        7,
        [full, jax.ShapeDtypeStruct((bands, 4 * rows), F32)],
        [factors, pltpu.VMEM(moved.shape, F32), pltpu.SemaphoreType.DMA((directions,))],
        [HBM, VMEM],
    )(moved, energy, wind, sea, west, east, band_rows.reshape(1, bands))
    count = lax.axis_size("gx")
    spread = lax.all_to_all(local.reshape(count, bands // count, 4 * rows), "gx", 0, 0)
    spread = spread.reshape(count, bands // count, 4, rows)
    ocean = jnp.transpose(spread, (2, 1, 0, 3)).reshape(4, bands // count, count * rows)
    return (spectrum_next, ocean)


def solution(mesh):
    placed = (
        P(None, None, ("member", "gx"), None),
        P(None, ("member", "gx"), None),
        P("gx", None),
        P(),
    )
    return jax.shard_map(
        per_device,
        mesh=mesh,
        in_specs=placed,
        out_specs=(P(None, None, ("member", "gx"), None), P(None, "gx", "member")),
        check_vma=False,
    )
```

```python
import math

import jax
import jax.numpy as jnp
from jax import lax
from jax.experimental import pallas as pl
from jax.experimental.pallas import tpu as pltpu
from jax.sharding import PartitionSpec as P

VMEM = pl.BlockSpec(memory_space=pltpu.VMEM)
HBM = pl.BlockSpec(memory_space=pltpu.HBM)
LIMIT = 20 * 1024 * 1024
STEPS = 3
F32 = jnp.float32


def passed_along(value, steps):
    count = lax.axis_size("gx")
    pairs = [(source, (source + steps) % count) for source in range(count)]
    return lax.ppermute(value, "gx", pairs)


def shrink(level):
    return 0.45 * 1.1 ** (-level)


def wind_factor(level):
    return 0.05 * 2.0 * math.pi * 0.0418 * 1.1**level / 9.81


def quadrants(directions):
    quarter = directions // 4
    return (
        (0, True, True, 0),
        (quarter, False, True, 0),
        (2 * quarter, False, False, quarter),
        (3 * quarter, True, False, quarter),
    )


def growth_of(ratio, level):
    return jnp.clip(ratio * wind_factor(level) - 0.05, 0.0, 0.2)


def damping_ratio(energy_sum, sea, bins):
    energy = sea * energy_sum * (1.0 / bins)
    return energy / (0.5 + energy)


def directions_loop(directions, start, body, shape, state):
    delta = 2.0 * math.pi / directions
    turn_c, turn_s = math.cos(delta), math.sin(delta)
    first = (start + 0.5) * delta

    def step(place, carry):
        cosine, sine, state = carry
        state = body(place, cosine, sine, state)
        return cosine * turn_c - sine * turn_s, sine * turn_c + cosine * turn_s, state

    begin = (jnp.full(shape, math.cos(first), F32), jnp.full(shape, math.sin(first), F32), state)
    return lax.fori_loop(0, directions // 4, step, begin)[2]


def flow(cosine, sine, eastward, northward):
    shape = cosine.shape
    row = lax.broadcasted_iota(jnp.int32, shape, 0)
    lane = lax.broadcasted_iota(jnp.int32, shape, 1)
    edge_row = 0 if eastward else shape[0] - 1
    edge_lane = 0 if northward else shape[1] - 1
    pace_x, pace_y = jnp.abs(cosine), jnp.abs(sine)
    inner_x = jnp.where(row == edge_row, 0.0, pace_x)
    halo_x = jnp.where(row == edge_row, pace_x, 0.0)
    inner_y = jnp.where(lane == edge_lane, 0.0, pace_y)
    return inner_x, halo_x, inner_y, pace_x + pace_y


def advect(cell, inner_x, inner_y, both, eastward, northward, level):
    rows, lanes = cell.shape
    up_x = pltpu.roll(cell, 1 if eastward else rows - 1, 0)
    up_y = pltpu.roll(cell, 1 if northward else lanes - 1, 1)
    return cell + shrink(level) * (inner_x * up_x + inner_y * up_y - both * cell)


def is_odd():
    return lax.axis_index("gx") % 2 == 1


def store_sends(near, far, place, eastward_part, westward_part):
    odd = is_odd()
    near[place] = jnp.where(odd, westward_part, eastward_part)
    far[place] = jnp.where(odd, eastward_part, westward_part)


def column_of(block, column):
    levels, rows, lanes = block.shape
    return block.reshape(levels * rows, lanes)[pl.ds(column, levels, stride=rows), :]


def columns_kernel(spectrum, near, far, staged, sems):
    directions, levels, rows, lanes = spectrum.shape
    quarter = directions // 4
    order = []
    for n in range(quarter):
        order += [(n, quarter + n, n), (3 * quarter + n, 2 * quarter + n, quarter + n)]

    def in_copy(index):
        return pltpu.make_async_copy(spectrum.at[index], staged.at[index], sems.at[index])

    for east, west, _ in order:
        in_copy(east).start()
        in_copy(west).start()
    for east, west, place in order:
        in_copy(east).wait()
        in_copy(west).wait()
        store_sends(near, far, place, column_of(staged.at[east], rows - 1), column_of(staged.at[west], 0))


def first_kernel(spectrum, advected, energy, edge_east, edge_west, staged, sems):
    directions, levels, rows, lanes = spectrum.shape
    total = jnp.zeros((rows, lanes), F32)

    def in_copy(index):
        return pltpu.make_async_copy(spectrum.at[index], staged.at[index], sems.at[index])

    def begin(index, _):
        in_copy(index).start()
        return 0

    lax.fori_loop(0, directions, begin, 0)
    for start, eastward, northward, place in quadrants(directions):
        edge = edge_east if eastward else edge_west
        column = rows - 1 if eastward else 0

        def body(n, cosine, sine, total, start=start, eastward=eastward, northward=northward, place=place, edge=edge, column=column):
            inner_x, _, inner_y, both = flow(cosine, sine, eastward, northward)
            in_copy(start + n).wait()
            for level in range(levels):
                cell = staged[start + n, level]
                moved = advect(cell, inner_x, inner_y, both, eastward, northward, level)
                advected[start + n, level] = moved
                total = total + moved
            edge[place + n] = column_of(advected.at[start + n], column)
            return total

        total = directions_loop(directions, start, body, (rows, lanes), total)
    energy[...] = total


def fill_factors(factors, energy, sea, bins, levels):
    ratio = damping_ratio(energy[...], sea[...], bins)
    for level in range(levels):
        weight = (level + 1.0) / levels
        factors[level] = sea[...] / (1.0 + (0.3 * weight * weight) * ratio)


def next_kernel(before, energy_in, wind, sea, from_west, from_east, advected, energy, edge_east, edge_west, factors):
    directions, levels, rows, lanes = before.shape
    fill_factors(factors, energy_in, sea, directions * levels, levels)
    total = jnp.zeros((rows, lanes), F32)
    for start, eastward, northward, place in quadrants(directions):
        halo = from_west if eastward else from_east
        sent = edge_east if eastward else edge_west
        column = rows - 1 if eastward else 0

        def body(n, cosine, sine, total, start=start, eastward=eastward, northward=northward, place=place, halo=halo, sent=sent, column=column):
            inner_x, halo_x, inner_y, both = flow(cosine, sine, eastward, northward)
            ratio = wind[0] * cosine + wind[1] * sine
            for level in range(levels):
                edge = jnp.broadcast_to(halo[place + n, pl.ds(level, 1), :], (rows, lanes))
                cell = before[start + n, level] + (shrink(level) * halo_x) * edge
                cell = cell * (1.0 + growth_of(ratio, level)) * factors[level]
                moved = advect(cell, inner_x, inner_y, both, eastward, northward, level)
                advected[start + n, level] = moved
                total = total + moved
            sent[place + n] = column_of(advected.at[start + n], column)
            return total

        total = directions_loop(directions, start, body, (rows, lanes), total)
    energy[...] = total


def last_kernel(before, energy_in, wind, sea, from_west, from_east, bands, spectrum, fields, factors, staged, sems):
    directions, levels, rows, lanes = before.shape
    quarter = directions // 4
    fill_factors(factors, energy_in, sea, directions * levels, levels)
    zero = jnp.zeros((rows, lanes), F32)
    sums = (zero, zero, zero, zero)

    def out_copy(index):
        return pltpu.make_async_copy(staged.at[index], spectrum.at[index], sems.at[index])

    for start, eastward, northward, place in quadrants(directions):
        halo = from_west if eastward else from_east

        def body(n, cosine, sine, sums, start=start, eastward=eastward, northward=northward, place=place, halo=halo):
            _, halo_x, _, _ = flow(cosine, sine, eastward, northward)
            ratio = wind[0] * cosine + wind[1] * sine
            input_sum, current_sum = zero, zero
            for level in range(levels):
                weight = (level + 1.0) / levels
                edge = jnp.broadcast_to(halo[place + n, pl.ds(level, 1), :], (rows, lanes))
                moved = before[start + n, level] + (shrink(level) * halo_x) * edge
                growth = growth_of(ratio, level)
                gained = growth * moved
                cell = (moved + gained) * factors[level]
                staged[start + n, level] = cell
                input_sum = input_sum + weight * gained
                current_sum = current_sum + weight * cell
            out_copy(start + n).start()
            return (
                sums[0] + cosine * input_sum,
                sums[1] + sine * input_sum,
                sums[2] + cosine * current_sum,
                sums[3] + sine * current_sum,
            )

        sums = directions_loop(directions, start, body, (rows, lanes), sums)
    scale = 3.0 / math.sqrt(directions * levels)
    mask = sea[...] * scale
    parts = [sums[0] * mask, sums[1] * mask, sums[2] * scale, sums[3] * scale]
    spare = fields.shape[-1] - 4 * rows
    if spare:
        parts.append(jnp.zeros((spare, lanes), F32))
    stacked = jnp.concatenate(parts, axis=0)
    wanted = jnp.broadcast_to(bands[...], (lanes, bands.shape[1]))
    choose = (lax.broadcasted_iota(jnp.int32, wanted.shape, 0) == wanted).astype(F32)
    picked = jnp.dot(stacked, choose, precision=lax.Precision.HIGHEST, preferred_element_type=F32)
    fields[...] = picked.T.reshape(fields.shape)

    def finish(index, _):
        out_copy(index).wait()
        return 0

    lax.fori_loop(0, directions, finish, 0)


def by_level(levels, lanes, function):
    level = lax.broadcasted_iota(jnp.int32, (levels, lanes), 0).astype(F32)
    return function(level)


def side_angles(directions, eastward):
    listed = []
    for start, east, northward, place in quadrants(directions):
        if east == eastward:
            for n in range(directions // 4):
                angle = (start + n + 0.5) * (2.0 * math.pi / directions)
                listed.append((place + n, math.cos(angle), math.sin(angle), northward))
    return listed


def growth_factor(levels, lanes):
    power = by_level(levels, lanes, lambda level: jnp.exp(level * math.log(1.1)))
    return power * wind_factor(0)


def halo_energy(halo, paces, directions, eastward):
    levels, lanes = paces.shape
    total = jnp.zeros((levels, lanes), F32)
    for place, cosine, _, _ in side_angles(directions, eastward):
        total = total + abs(cosine) * halo[place]
    return jnp.sum(total * paces, axis=0, keepdims=True)


def with_halo_energy(partial, west_sum, east_sum):
    row = lax.broadcasted_iota(jnp.int32, partial.shape, 0)
    add = jnp.where(row == 0, west_sum, 0.0) + jnp.where(row == partial.shape[0] - 1, east_sum, 0.0)
    return partial + add


def paces_of(levels, lanes):
    return by_level(levels, lanes, lambda level: 0.45 * jnp.exp(level * -math.log(1.1)))


def pick(array, row):
    return array[row : row + 1, :]


def edge_kernel(partial, wind, sea, near_in, far_in, edge_east, edge_west,
                from_west, from_east, energy, near_out=None, far_out=None):
    half, levels, lanes = near_in.shape
    rows = partial.shape[0]
    directions = 2 * half
    odd = is_odd()
    paces = paces_of(levels, lanes)
    for place in range(half):
        near, far = near_in[place], far_in[place]
        from_west[place] = jnp.where(odd, near, far)
        from_east[place] = jnp.where(odd, far, near)
    west_sum = halo_energy(from_west, paces, directions, True)
    east_sum = halo_energy(from_east, paces, directions, False)
    full = with_halo_energy(partial[...], west_sum, east_sum)
    energy[...] = full
    if near_out is None:
        return
    winds = growth_factor(levels, lanes)
    weight = by_level(levels, lanes, lambda level: (level + 1.0) * (1.0 / levels))
    wind_x, wind_y, mask = wind[0], wind[1], sea[...]

    def next_edges(edges, column, eastward):
        ratio = damping_ratio(pick(full, column), pick(mask, column), directions * levels)
        factor = pick(mask, column) / (1.0 + 0.3 * weight * weight * ratio)
        result = []
        for place, cosine, sine, _ in sorted(side_angles(directions, eastward)):
            pace = pick(wind_x, column) * cosine + pick(wind_y, column) * sine
            growth = jnp.clip(pace * winds - 0.05, 0.0, 0.2)
            result.append(edges[place] * (1.0 + growth) * factor)
        return result

    easts = next_edges(edge_east, rows - 1, True)
    wests = next_edges(edge_west, 0, False)
    for place in range(half):
        store_sends(near_out, far_out, place, easts[place], wests[place])


def last_edge_kernel(partial, near_in, far_in, from_west, from_east, energy):
    edge_kernel(partial, None, None, near_in, far_in, None, None, from_west, from_east, energy)


def ocean_kernel(parts, ocean):
    count, bands, lanes = parts.shape
    fields, _, width = ocean.shape
    rows = width // count
    per_tile = lanes // rows
    group = lax.broadcasted_iota(jnp.int32, (bands, lanes), 1) // rows
    for tile in range(width // lanes):
        for field in range(fields):
            value = jnp.zeros((bands, lanes), F32)
            for slot in range(per_tile):
                shift = ((slot - field) * rows) % lanes
                part = parts[tile * per_tile + slot]
                part = pltpu.roll(part, shift, 1) if shift else part
                value = jnp.where(group == slot, part, value)
            ocean[field, :, tile * lanes : (tile + 1) * lanes] = value


def exchanged(near, far):
    count = lax.axis_size("gx")
    inside = [(source, source ^ 1) for source in range(count)]
    across = [(source, (source + (1 if source % 2 else -1)) % count) for source in range(count)]
    return lax.ppermute(far, "gx", across), lax.ppermute(near, "gx", inside)


def per_device(spectrum, wind, land_sea, band_rows):
    directions, levels, rows, lanes = spectrum.shape
    half = directions // 2
    bands = band_rows.shape[0]
    count = lax.axis_size("gx")
    sea = land_sea.astype(F32)
    full = jax.ShapeDtypeStruct(spectrum.shape, F32)
    plane = jax.ShapeDtypeStruct((rows, lanes), F32)
    column = jax.ShapeDtypeStruct((half, levels, lanes), F32)
    factors = pltpu.VMEM((levels, rows, lanes), F32)
    staging = [pltpu.VMEM(spectrum.shape, F32), pltpu.SemaphoreType.DMA((directions,))]

    def call(kernel, ins, outs, scratch=(), out_specs=None):
        return pl.pallas_call(
            kernel,
            in_specs=ins,
            out_specs=[VMEM] * len(outs) if out_specs is None else out_specs,
            out_shape=outs,
            scratch_shapes=list(scratch),
            compiler_params=pltpu.CompilerParams(vmem_limit_bytes=LIMIT),
            name=kernel.__name__,
        )

    near, far = call(columns_kernel, [HBM], [column] * 2, staging)(spectrum)
    far, near = exchanged(near, far)
    moved, partial, edge_east, edge_west = call(first_kernel, [HBM], [full, plane, column, column], staging)(spectrum)
    edges = call(edge_kernel, [VMEM] * 7, [column, column, plane, column, column])
    step = call(next_kernel, [VMEM] * 6, [full, plane, column, column], [factors])
    for _ in range(STEPS - 1):
        west, east, energy, near, far = edges(partial, wind, sea, near, far, edge_east, edge_west)
        far, near = exchanged(near, far)
        moved, partial, edge_east, edge_west = step(moved, energy, wind, sea, west, east)
    west, east, energy = call(last_edge_kernel, [VMEM] * 3, [column, column, plane])(partial, near, far)
    block = jax.ShapeDtypeStruct((count, bands // count, lanes), F32)
    spectrum_next, local = call(last_kernel, [VMEM] * 7, [full, block], [factors] + staging, [HBM, VMEM])(
        moved, energy, wind, sea, west, east, band_rows.reshape(1, bands)
    )
    spread = lax.all_to_all(local, "gx", 0, 0)
    ocean = call(ocean_kernel, [VMEM], jax.ShapeDtypeStruct((4, bands // count, count * rows), F32), (), VMEM)(spread)
    return (spectrum_next, ocean)


def solution(mesh):
    placed = (
        P(None, None, ("member", "gx"), None),
        P(None, ("member", "gx"), None),
        P("gx", None),
        P(),
    )
    return jax.shard_map(
        per_device,
        mesh=mesh,
        in_specs=placed,
        out_specs=(P(None, None, ("member", "gx"), None), P(None, "gx", "member")),
        check_vma=False,
    )
```

```python
import math

import jax
import jax.numpy as jnp
from jax import lax
from jax.experimental import pallas as pl
from jax.experimental.pallas import tpu as pltpu
from jax.sharding import PartitionSpec as P

VMEM = pl.BlockSpec(memory_space=pltpu.VMEM)
HBM = pl.BlockSpec(memory_space=pltpu.HBM)
LIMIT = 20 * 1024 * 1024
STEPS = 3
F32 = jnp.float32


def passed_along(value, steps):
    count = lax.axis_size("gx")
    pairs = [(source, (source + steps) % count) for source in range(count)]
    return lax.ppermute(value, "gx", pairs)


def shrink(level):
    return 0.45 * 1.1 ** (-level)


def wind_factor(level):
    return 0.05 * 2.0 * math.pi * 0.0418 * 1.1**level / 9.81


def quadrants(directions):
    quarter = directions // 4
    return (
        (0, True, True, 0),
        (quarter, False, True, 0),
        (2 * quarter, False, False, quarter),
        (3 * quarter, True, False, quarter),
    )


def growth_of(ratio, level):
    return jnp.clip(ratio * wind_factor(level) - 0.05, 0.0, 0.2)


def damping_ratio(energy_sum, sea, bins):
    energy = sea * energy_sum * (1.0 / bins)
    return energy / (0.5 + energy)


def directions_loop(directions, start, body, shape, state):
    delta = 2.0 * math.pi / directions
    turn_c, turn_s = math.cos(delta), math.sin(delta)
    first = (start + 0.5) * delta

    def step(place, carry):
        cosine, sine, state = carry
        state = body(place, cosine, sine, state)
        return cosine * turn_c - sine * turn_s, sine * turn_c + cosine * turn_s, state

    begin = (jnp.full(shape, math.cos(first), F32), jnp.full(shape, math.sin(first), F32), state)
    return lax.fori_loop(0, directions // 4, step, begin)[2]


def flow(cosine, sine, eastward, northward):
    shape = cosine.shape
    row = lax.broadcasted_iota(jnp.int32, shape, 0)
    lane = lax.broadcasted_iota(jnp.int32, shape, 1)
    edge_row = 0 if eastward else shape[0] - 1
    edge_lane = 0 if northward else shape[1] - 1
    pace_x, pace_y = jnp.abs(cosine), jnp.abs(sine)
    inner_x = jnp.where(row == edge_row, 0.0, pace_x)
    halo_x = jnp.where(row == edge_row, pace_x, 0.0)
    inner_y = jnp.where(lane == edge_lane, 0.0, pace_y)
    return inner_x, halo_x, inner_y, pace_x + pace_y


def advect(cell, inner_x, inner_y, both, eastward, northward, level):
    rows, lanes = cell.shape
    up_x = pltpu.roll(cell, 1 if eastward else rows - 1, 0)
    up_y = pltpu.roll(cell, 1 if northward else lanes - 1, 1)
    return cell + shrink(level) * (inner_x * up_x + inner_y * up_y - both * cell)


def is_odd():
    return lax.axis_index("gx") % 2 == 1


def store_sends(near, far, place, eastward_part, westward_part):
    odd = is_odd()
    near[place] = jnp.where(odd, westward_part, eastward_part)
    far[place] = jnp.where(odd, eastward_part, westward_part)


def column_of(block, column):
    levels, rows, lanes = block.shape
    return block.reshape(levels * rows, lanes)[pl.ds(column, levels, stride=rows), :]


def columns_kernel(spectrum, near, far):
    directions, levels, rows, lanes = spectrum.shape
    quarter = directions // 4

    def move(n, _):
        for east, west, place in ((0, quarter, 0), (3 * quarter, 2 * quarter, quarter)):
            eastward_part = column_of(spectrum.at[east + n], rows - 1)
            store_sends(near, far, place + n, eastward_part, column_of(spectrum.at[west + n], 0))
        return 0

    lax.fori_loop(0, quarter, move, 0)


def first_kernel(spectrum, advected, energy, edge_east, edge_west):
    directions, levels, rows, lanes = spectrum.shape
    total = jnp.zeros((rows, lanes), F32)
    for start, eastward, northward, place in quadrants(directions):
        edge = edge_east if eastward else edge_west
        column = rows - 1 if eastward else 0

        def body(n, cosine, sine, total, start=start, eastward=eastward, northward=northward, place=place, edge=edge, column=column):
            inner_x, _, inner_y, both = flow(cosine, sine, eastward, northward)
            for level in range(levels):
                cell = spectrum[start + n, level]
                moved = advect(cell, inner_x, inner_y, both, eastward, northward, level)
                advected[start + n, level] = moved
                total = total + moved
            edge[place + n] = column_of(advected.at[start + n], column)
            return total

        total = directions_loop(directions, start, body, (rows, lanes), total)
    energy[...] = total


def fill_factors(factors, energy, sea, bins, levels):
    ratio = damping_ratio(energy[...], sea[...], bins)
    for level in range(levels):
        weight = (level + 1.0) / levels
        factors[level] = sea[...] / (1.0 + (0.3 * weight * weight) * ratio)


def next_kernel(before, energy_in, wind, sea, from_west, from_east, advected, energy, edge_east, edge_west, factors):
    directions, levels, rows, lanes = before.shape
    fill_factors(factors, energy_in, sea, directions * levels, levels)
    total = jnp.zeros((rows, lanes), F32)
    for start, eastward, northward, place in quadrants(directions):
        halo = from_west if eastward else from_east
        sent = edge_east if eastward else edge_west
        column = rows - 1 if eastward else 0

        def body(n, cosine, sine, total, start=start, eastward=eastward, northward=northward, place=place, halo=halo, sent=sent, column=column):
            inner_x, halo_x, inner_y, both = flow(cosine, sine, eastward, northward)
            ratio = wind[0] * cosine + wind[1] * sine
            for level in range(levels):
                edge = jnp.broadcast_to(halo[place + n, pl.ds(level, 1), :], (rows, lanes))
                cell = before[start + n, level] + (shrink(level) * halo_x) * edge
                cell = cell * (1.0 + growth_of(ratio, level)) * factors[level]
                moved = advect(cell, inner_x, inner_y, both, eastward, northward, level)
                advected[start + n, level] = moved
                total = total + moved
            if sent is not None:
                sent[place + n] = column_of(advected.at[start + n], column)
            return total

        total = directions_loop(directions, start, body, (rows, lanes), total)
    energy[...] = total


def plain_next_kernel(before, energy_in, wind, sea, from_west, from_east, advected, energy, factors):
    next_kernel(before, energy_in, wind, sea, from_west, from_east, advected, energy, None, None, factors)


def last_kernel(before, energy_in, wind, sea, from_west, from_east, bands, spectrum, fields, factors, staged, sems):
    directions, levels, rows, lanes = before.shape
    quarter = directions // 4
    fill_factors(factors, energy_in, sea, directions * levels, levels)
    zero = jnp.zeros((rows, lanes), F32)
    sums = (zero, zero, zero, zero)

    def out_copy(index):
        return pltpu.make_async_copy(staged.at[index], spectrum.at[index], sems.at[index])

    for start, eastward, northward, place in quadrants(directions):
        halo = from_west if eastward else from_east

        def body(n, cosine, sine, sums, start=start, eastward=eastward, northward=northward, place=place, halo=halo):
            _, halo_x, _, _ = flow(cosine, sine, eastward, northward)
            ratio = wind[0] * cosine + wind[1] * sine
            input_sum, current_sum = zero, zero
            for level in range(levels):
                weight = (level + 1.0) / levels
                edge = jnp.broadcast_to(halo[place + n, pl.ds(level, 1), :], (rows, lanes))
                moved = before[start + n, level] + (shrink(level) * halo_x) * edge
                growth = growth_of(ratio, level)
                gained = growth * moved
                cell = (moved + gained) * factors[level]
                staged[start + n, level] = cell
                input_sum = input_sum + weight * gained
                current_sum = current_sum + weight * cell
            out_copy(start + n).start()
            return (
                sums[0] + cosine * input_sum,
                sums[1] + sine * input_sum,
                sums[2] + cosine * current_sum,
                sums[3] + sine * current_sum,
            )

        sums = directions_loop(directions, start, body, (rows, lanes), sums)
    scale = 3.0 / math.sqrt(directions * levels)
    mask = sea[...] * scale
    parts = [sums[0] * mask, sums[1] * mask, sums[2] * scale, sums[3] * scale]
    spare = fields.shape[-1] - 4 * rows
    if spare:
        parts.append(jnp.zeros((spare, lanes), F32))
    stacked = jnp.concatenate(parts, axis=0)
    wanted = jnp.broadcast_to(bands[...], (lanes, bands.shape[1]))
    choose = (lax.broadcasted_iota(jnp.int32, wanted.shape, 0) == wanted).astype(F32)
    picked = jnp.dot(stacked, choose, precision=lax.Precision.HIGHEST, preferred_element_type=F32)
    fields[...] = picked.T.reshape(fields.shape)

    def finish(index, _):
        out_copy(index).wait()
        return 0

    lax.fori_loop(0, directions, finish, 0)


def by_level(levels, lanes, function):
    level = lax.broadcasted_iota(jnp.int32, (levels, lanes), 0).astype(F32)
    return function(level)


def side_angles(directions, eastward):
    listed = []
    for start, east, northward, place in quadrants(directions):
        if east == eastward:
            for n in range(directions // 4):
                angle = (start + n + 0.5) * (2.0 * math.pi / directions)
                listed.append((place + n, math.cos(angle), math.sin(angle), northward))
    return listed


def growth_factor(levels, lanes):
    power = by_level(levels, lanes, lambda level: jnp.exp(level * math.log(1.1)))
    return power * wind_factor(0)


def halo_energy(halo, paces, directions, eastward):
    levels, lanes = paces.shape
    total = jnp.zeros((levels, lanes), F32)
    for place, cosine, _, _ in side_angles(directions, eastward):
        total = total + abs(cosine) * halo[place]
    return jnp.sum(total * paces, axis=0, keepdims=True)


def with_halo_energy(partial, west_sum, east_sum):
    row = lax.broadcasted_iota(jnp.int32, partial.shape, 0)
    add = jnp.where(row == 0, west_sum, 0.0) + jnp.where(row == partial.shape[0] - 1, east_sum, 0.0)
    return partial + add


def paces_of(levels, lanes):
    return by_level(levels, lanes, lambda level: 0.45 * jnp.exp(level * -math.log(1.1)))


def pick(array, row):
    return array[row : row + 1, :]


def edge_kernel(partial, wind, sea, near_in, far_in, edge_east, edge_west,
                from_west, from_east, energy, near_out=None, far_out=None):
    half, levels, lanes = near_in.shape
    rows = partial.shape[0]
    directions = 2 * half
    odd = is_odd()
    paces = paces_of(levels, lanes)
    for place in range(half):
        near, far = near_in[place], far_in[place]
        from_west[place] = jnp.where(odd, near, far)
        from_east[place] = jnp.where(odd, far, near)
    west_sum = halo_energy(from_west, paces, directions, True)
    east_sum = halo_energy(from_east, paces, directions, False)
    full = with_halo_energy(partial[...], west_sum, east_sum)
    energy[...] = full
    if near_out is None:
        return
    winds = growth_factor(levels, lanes)
    weight = by_level(levels, lanes, lambda level: (level + 1.0) * (1.0 / levels))
    wind_x, wind_y, mask = wind[0], wind[1], sea[...]

    def next_edges(edges, column, eastward):
        ratio = damping_ratio(pick(full, column), pick(mask, column), directions * levels)
        factor = pick(mask, column) / (1.0 + 0.3 * weight * weight * ratio)
        result = []
        for place, cosine, sine, _ in sorted(side_angles(directions, eastward)):
            pace = pick(wind_x, column) * cosine + pick(wind_y, column) * sine
            growth = jnp.clip(pace * winds - 0.05, 0.0, 0.2)
            result.append(edges[place] * (1.0 + growth) * factor)
        return result

    easts = next_edges(edge_east, rows - 1, True)
    wests = next_edges(edge_west, 0, False)
    for place in range(half):
        store_sends(near_out, far_out, place, easts[place], wests[place])


def last_edge_kernel(partial, near_in, far_in, from_west, from_east, energy):
    edge_kernel(partial, None, None, near_in, far_in, None, None, from_west, from_east, energy)


def ocean_kernel(parts, ocean):
    count, bands, lanes = parts.shape
    fields, _, width = ocean.shape
    rows = width // count
    per_tile = lanes // rows
    group = lax.broadcasted_iota(jnp.int32, (bands, lanes), 1) // rows
    for tile in range(width // lanes):
        for field in range(fields):
            value = jnp.zeros((bands, lanes), F32)
            for slot in range(per_tile):
                shift = ((slot - field) * rows) % lanes
                part = parts[tile * per_tile + slot]
                part = pltpu.roll(part, shift, 1) if shift else part
                value = jnp.where(group == slot, part, value)
            ocean[field, :, tile * lanes : (tile + 1) * lanes] = value


def exchanged(near, far):
    count = lax.axis_size("gx")
    inside = [(source, source ^ 1) for source in range(count)]
    across = [(source, (source + (1 if source % 2 else -1)) % count) for source in range(count)]
    return lax.ppermute(far, "gx", across), lax.ppermute(near, "gx", inside)


def per_device(spectrum, wind, land_sea, band_rows):
    directions, levels, rows, lanes = spectrum.shape
    half = directions // 2
    bands = band_rows.shape[0]
    count = lax.axis_size("gx")
    sea = land_sea.astype(F32)
    full = jax.ShapeDtypeStruct(spectrum.shape, F32)
    plane = jax.ShapeDtypeStruct((rows, lanes), F32)
    column = jax.ShapeDtypeStruct((half, levels, lanes), F32)
    factors = pltpu.VMEM((levels, rows, lanes), F32)
    staging = [pltpu.VMEM(spectrum.shape, F32), pltpu.SemaphoreType.DMA((directions,))]

    def call(kernel, ins, outs, scratch=(), out_specs=None):
        return pl.pallas_call(
            kernel,
            in_specs=ins,
            out_specs=[VMEM] * len(outs) if out_specs is None else out_specs,
            out_shape=outs,
            scratch_shapes=list(scratch),
            compiler_params=pltpu.CompilerParams(vmem_limit_bytes=LIMIT),
            name=kernel.__name__,
        )

    near, far = call(columns_kernel, [VMEM], [column] * 2)(spectrum)
    far, near = exchanged(near, far)
    moved, partial, edge_east, edge_west = call(first_kernel, [VMEM], [full, plane, column, column])(spectrum)
    edges = call(edge_kernel, [VMEM] * 7, [column, column, plane, column, column])
    step = call(next_kernel, [VMEM] * 6, [full, plane, column, column], [factors])
    plain_step = call(plain_next_kernel, [VMEM] * 6, [full, plane], [factors])
    for index in range(1, STEPS):
        west, east, energy, near, far = edges(partial, wind, sea, near, far, edge_east, edge_west)
        far, near = exchanged(near, far)
        if index == STEPS - 1:
            moved, partial = plain_step(moved, energy, wind, sea, west, east)
        else:
            moved, partial, edge_east, edge_west = step(moved, energy, wind, sea, west, east)
    west, east, energy = call(last_edge_kernel, [VMEM] * 3, [column, column, plane])(partial, near, far)
    block = jax.ShapeDtypeStruct((count, bands // count, lanes), F32)
    spectrum_next, local = call(last_kernel, [VMEM] * 7, [full, block], [factors] + staging, [HBM, VMEM])(
        moved, energy, wind, sea, west, east, band_rows.reshape(1, bands)
    )
    spread = lax.all_to_all(local, "gx", 0, 0)
    ocean = call(ocean_kernel, [VMEM], jax.ShapeDtypeStruct((4, bands // count, count * rows), F32), (), VMEM)(spread)
    return (spectrum_next, ocean)


def solution(mesh):
    placed = (
        P(None, None, ("member", "gx"), None),
        P(None, ("member", "gx"), None),
        P("gx", None),
        P(),
    )
    return jax.shard_map(
        per_device,
        mesh=mesh,
        in_specs=placed,
        out_specs=(P(None, None, ("member", "gx"), None), P(None, "gx", "member")),
        check_vma=False,
    )
```

```python
import math

import jax
import jax.numpy as jnp
from jax import lax
from jax.experimental import pallas as pl
from jax.experimental.pallas import tpu as pltpu
from jax.sharding import PartitionSpec as P

VMEM = pl.BlockSpec(memory_space=pltpu.VMEM)
HBM = pl.BlockSpec(memory_space=pltpu.HBM)
LIMIT = 20 * 1024 * 1024
STEPS = 3
F32 = jnp.float32


def passed_along(value, steps):
    count = lax.axis_size("gx")
    pairs = [(source, (source + steps) % count) for source in range(count)]
    return lax.ppermute(value, "gx", pairs)


def shrink(level):
    return 0.45 * 1.1 ** (-level)


def wind_factor(level):
    return 0.05 * 2.0 * math.pi * 0.0418 * 1.1**level / 9.81


def quadrants(directions):
    quarter = directions // 4
    return (
        (0, True, True, 0),
        (quarter, False, True, 0),
        (2 * quarter, False, False, quarter),
        (3 * quarter, True, False, quarter),
    )


def growth_of(ratio, level):
    return jnp.clip(ratio * wind_factor(level) - 0.05, 0.0, 0.2)


def damping_ratio(energy_sum, sea, bins):
    energy = sea * energy_sum * (1.0 / bins)
    return energy / (0.5 + energy)


def directions_loop(directions, start, body, shape, state):
    delta = 2.0 * math.pi / directions
    turn_c, turn_s = math.cos(delta), math.sin(delta)
    first = (start + 0.5) * delta

    def step(place, carry):
        cosine, sine, state = carry
        state = body(place, cosine, sine, state)
        return cosine * turn_c - sine * turn_s, sine * turn_c + cosine * turn_s, state

    begin = (jnp.full(shape, math.cos(first), F32), jnp.full(shape, math.sin(first), F32), state)
    return lax.fori_loop(0, directions // 4, step, begin)[2]


def flow(cosine, sine, eastward, northward):
    shape = cosine.shape
    row = lax.broadcasted_iota(jnp.int32, shape, 0)
    lane = lax.broadcasted_iota(jnp.int32, shape, 1)
    edge_row = 0 if eastward else shape[0] - 1
    edge_lane = 0 if northward else shape[1] - 1
    pace_x, pace_y = jnp.abs(cosine), jnp.abs(sine)
    inner_x = jnp.where(row == edge_row, 0.0, pace_x)
    halo_x = jnp.where(row == edge_row, 1.0, 0.0)
    inner_y = jnp.where(lane == edge_lane, 0.0, pace_y)
    return inner_x, halo_x, inner_y, pace_x + pace_y


def advect(cell, inner_x, inner_y, both, eastward, northward, level):
    rows, lanes = cell.shape
    up_x = pltpu.roll(cell, 1 if eastward else rows - 1, 0)
    up_y = pltpu.roll(cell, 1 if northward else lanes - 1, 1)
    return cell + shrink(level) * (inner_x * up_x + inner_y * up_y - both * cell)


def is_odd():
    return lax.axis_index("gx") % 2 == 1


def store_sends(near, far, place, eastward_part, westward_part):
    odd = is_odd()
    near[place] = jnp.where(odd, westward_part, eastward_part)
    far[place] = jnp.where(odd, eastward_part, westward_part)


def column_of(block, column):
    levels, rows, lanes = block.shape
    return block.reshape(levels * rows, lanes)[pl.ds(column, levels, stride=rows), :]


def columns_kernel(spectrum, near, far):
    directions, levels, rows, lanes = spectrum.shape
    quarter = directions // 4

    def move(n, _):
        for east, west, place in ((0, quarter, 0), (3 * quarter, 2 * quarter, quarter)):
            eastward_part = column_of(spectrum.at[east + n], rows - 1)
            store_sends(near, far, place + n, eastward_part, column_of(spectrum.at[west + n], 0))
        return 0

    lax.fori_loop(0, quarter, move, 0)


def first_kernel(spectrum, advected, energy, edge_east, edge_west):
    directions, levels, rows, lanes = spectrum.shape
    total = jnp.zeros((rows, lanes), F32)
    for start, eastward, northward, place in quadrants(directions):
        edge = edge_east if eastward else edge_west
        column = rows - 1 if eastward else 0

        def body(n, cosine, sine, total, start=start, eastward=eastward, northward=northward, place=place, edge=edge, column=column):
            inner_x, _, inner_y, both = flow(cosine, sine, eastward, northward)
            for level in range(levels):
                cell = spectrum[start + n, level]
                moved = advect(cell, inner_x, inner_y, both, eastward, northward, level)
                advected[start + n, level] = moved
                total = total + moved
            edge[place + n] = column_of(advected.at[start + n], column)
            return total

        total = directions_loop(directions, start, body, (rows, lanes), total)
    energy[...] = total


def fill_factors(factors, energy, sea, bins, levels):
    ratio = damping_ratio(energy[...], sea[...], bins)
    for level in range(levels):
        weight = (level + 1.0) / levels
        factors[level] = sea[...] / (1.0 + (0.3 * weight * weight) * ratio)


def next_kernel(before, energy_in, wind, sea, from_west, from_east, advected, energy, edge_east, edge_west, factors):
    directions, levels, rows, lanes = before.shape
    fill_factors(factors, energy_in, sea, directions * levels, levels)
    total = jnp.zeros((rows, lanes), F32)
    for start, eastward, northward, place in quadrants(directions):
        halo = from_west if eastward else from_east
        sent = edge_east if eastward else edge_west
        column = rows - 1 if eastward else 0

        def body(n, cosine, sine, total, start=start, eastward=eastward, northward=northward, place=place, halo=halo, sent=sent, column=column):
            inner_x, halo_x, inner_y, both = flow(cosine, sine, eastward, northward)
            ratio = wind[0] * cosine + wind[1] * sine
            for level in range(levels):
                edge = jnp.broadcast_to(halo[place + n, pl.ds(level, 1), :], (rows, lanes))
                cell = before[start + n, level] + halo_x * edge
                gain = jnp.clip(ratio * wind_factor(level) + 0.95, 1.0, 1.2)
                cell = cell * gain * factors[level]
                moved = advect(cell, inner_x, inner_y, both, eastward, northward, level)
                advected[start + n, level] = moved
                total = total + moved
            if sent is not None:
                sent[place + n] = column_of(advected.at[start + n], column)
            return total

        total = directions_loop(directions, start, body, (rows, lanes), total)
    energy[...] = total


def plain_next_kernel(before, energy_in, wind, sea, from_west, from_east, advected, energy, factors):
    next_kernel(before, energy_in, wind, sea, from_west, from_east, advected, energy, None, None, factors)


def last_kernel(before, energy_in, wind, sea, from_west, from_east, bands, spectrum, fields, factors, staged, sems):
    directions, levels, rows, lanes = before.shape
    quarter = directions // 4
    fill_factors(factors, energy_in, sea, directions * levels, levels)
    zero = jnp.zeros((rows, lanes), F32)
    sums = (zero, zero, zero, zero)

    def out_copy(index):
        return pltpu.make_async_copy(staged.at[index], spectrum.at[index], sems.at[index])

    for start, eastward, northward, place in quadrants(directions):
        halo = from_west if eastward else from_east

        def body(n, cosine, sine, sums, start=start, eastward=eastward, northward=northward, place=place, halo=halo):
            _, halo_x, _, _ = flow(cosine, sine, eastward, northward)
            ratio = wind[0] * cosine + wind[1] * sine
            input_sum, current_sum = zero, zero
            for level in range(levels):
                weight = (level + 1.0) / levels
                edge = jnp.broadcast_to(halo[place + n, pl.ds(level, 1), :], (rows, lanes))
                moved = before[start + n, level] + halo_x * edge
                growth = growth_of(ratio, level)
                gained = growth * moved
                cell = (moved + gained) * factors[level]
                staged[start + n, level] = cell
                input_sum = input_sum + weight * gained
                current_sum = current_sum + weight * cell
            out_copy(start + n).start()
            return (
                sums[0] + cosine * input_sum,
                sums[1] + sine * input_sum,
                sums[2] + cosine * current_sum,
                sums[3] + sine * current_sum,
            )

        sums = directions_loop(directions, start, body, (rows, lanes), sums)
    scale = 3.0 / math.sqrt(directions * levels)
    mask = sea[...] * scale
    parts = [sums[0] * mask, sums[1] * mask, sums[2] * scale, sums[3] * scale]
    spare = fields.shape[-1] - 4 * rows
    if spare:
        parts.append(jnp.zeros((spare, lanes), F32))
    stacked = jnp.concatenate(parts, axis=0)
    wanted = jnp.broadcast_to(bands[...], (lanes, bands.shape[1]))
    choose = (lax.broadcasted_iota(jnp.int32, wanted.shape, 0) == wanted).astype(F32)
    picked = jnp.dot(stacked, choose, precision=lax.Precision.HIGHEST, preferred_element_type=F32)
    fields[...] = picked.T.reshape(fields.shape)

    def finish(index, _):
        out_copy(index).wait()
        return 0

    lax.fori_loop(0, directions, finish, 0)


def by_level(levels, lanes, function):
    level = lax.broadcasted_iota(jnp.int32, (levels, lanes), 0).astype(F32)
    return function(level)


def side_angles(directions, eastward):
    listed = []
    for start, east, northward, place in quadrants(directions):
        if east == eastward:
            for n in range(directions // 4):
                angle = (start + n + 0.5) * (2.0 * math.pi / directions)
                listed.append((place + n, math.cos(angle), math.sin(angle), northward))
    return listed


def growth_factor(levels, lanes):
    power = by_level(levels, lanes, lambda level: jnp.exp(level * math.log(1.1)))
    return power * wind_factor(0)


def with_halo_energy(partial, west_sum, east_sum):
    row = lax.broadcasted_iota(jnp.int32, partial.shape, 0)
    add = jnp.where(row == 0, west_sum, 0.0) + jnp.where(row == partial.shape[0] - 1, east_sum, 0.0)
    return partial + add


def paces_of(levels, lanes):
    return by_level(levels, lanes, lambda level: 0.45 * jnp.exp(level * -math.log(1.1)))


def pick(array, row):
    return array[row : row + 1, :]


def edge_kernel(partial, wind, sea, near_in, far_in, edge_east, edge_west,
                from_west, from_east, energy, near_out=None, far_out=None):
    half, levels, lanes = near_in.shape
    rows = partial.shape[0]
    directions = 2 * half
    odd = is_odd()
    paces = paces_of(levels, lanes)
    sums = []
    for eastward, out in ((True, from_west), (False, from_east)):
        total = jnp.zeros((levels, lanes), F32)
        for place, cosine, _, _ in sorted(side_angles(directions, eastward)):
            first, second = (near_in, far_in) if eastward else (far_in, near_in)
            share = jnp.where(odd, first[place], second[place]) * (paces * abs(cosine))
            out[place] = share
            total = total + share
        sums.append(jnp.sum(total, axis=0, keepdims=True))
    west_sum, east_sum = sums
    full = with_halo_energy(partial[...], west_sum, east_sum)
    energy[...] = full
    if near_out is None:
        return
    winds = growth_factor(levels, lanes)
    weight = by_level(levels, lanes, lambda level: (level + 1.0) * (1.0 / levels))
    wind_x, wind_y, mask = wind[0], wind[1], sea[...]

    def next_edges(edges, column, eastward):
        ratio = damping_ratio(pick(full, column), pick(mask, column), directions * levels)
        factor = pick(mask, column) / (1.0 + 0.3 * weight * weight * ratio)
        result = []
        for place, cosine, sine, _ in sorted(side_angles(directions, eastward)):
            pace = pick(wind_x, column) * cosine + pick(wind_y, column) * sine
            growth = jnp.clip(pace * winds - 0.05, 0.0, 0.2)
            result.append(edges[place] * (1.0 + growth) * factor)
        return result

    easts = next_edges(edge_east, rows - 1, True)
    wests = next_edges(edge_west, 0, False)
    for place in range(half):
        store_sends(near_out, far_out, place, easts[place], wests[place])


def last_edge_kernel(partial, near_in, far_in, from_west, from_east, energy):
    edge_kernel(partial, None, None, near_in, far_in, None, None, from_west, from_east, energy)


def ocean_kernel(parts, ocean):
    count, bands, lanes = parts.shape
    fields, _, width = ocean.shape
    rows = width // count
    per_tile = lanes // rows
    group = lax.broadcasted_iota(jnp.int32, (bands, lanes), 1) // rows
    for tile in range(width // lanes):
        for field in range(fields):
            value = jnp.zeros((bands, lanes), F32)
            for slot in range(per_tile):
                shift = ((slot - field) * rows) % lanes
                part = parts[tile * per_tile + slot]
                part = pltpu.roll(part, shift, 1) if shift else part
                value = jnp.where(group == slot, part, value)
            ocean[field, :, tile * lanes : (tile + 1) * lanes] = value


def exchanged(near, far):
    count = lax.axis_size("gx")
    inside = [(source, source ^ 1) for source in range(count)]
    across = [(source, (source + (1 if source % 2 else -1)) % count) for source in range(count)]
    return lax.ppermute(far, "gx", across), lax.ppermute(near, "gx", inside)


def per_device(spectrum, wind, land_sea, band_rows):
    directions, levels, rows, lanes = spectrum.shape
    half = directions // 2
    bands = band_rows.shape[0]
    count = lax.axis_size("gx")
    sea = land_sea.astype(F32)
    full = jax.ShapeDtypeStruct(spectrum.shape, F32)
    plane = jax.ShapeDtypeStruct((rows, lanes), F32)
    column = jax.ShapeDtypeStruct((half, levels, lanes), F32)
    factors = pltpu.VMEM((levels, rows, lanes), F32)
    staging = [pltpu.VMEM(spectrum.shape, F32), pltpu.SemaphoreType.DMA((directions,))]

    def call(kernel, ins, outs, scratch=(), out_specs=None):
        return pl.pallas_call(
            kernel,
            in_specs=ins,
            out_specs=[VMEM] * len(outs) if out_specs is None else out_specs,
            out_shape=outs,
            scratch_shapes=list(scratch),
            compiler_params=pltpu.CompilerParams(vmem_limit_bytes=LIMIT),
            name=kernel.__name__,
        )

    near, far = call(columns_kernel, [VMEM], [column] * 2)(spectrum)
    far, near = exchanged(near, far)
    moved, partial, edge_east, edge_west = call(first_kernel, [VMEM], [full, plane, column, column])(spectrum)
    edges = call(edge_kernel, [VMEM] * 7, [column, column, plane, column, column])
    step = call(next_kernel, [VMEM] * 6, [full, plane, column, column], [factors])
    plain_step = call(plain_next_kernel, [VMEM] * 6, [full, plane], [factors])
    for index in range(1, STEPS):
        west, east, energy, near, far = edges(partial, wind, sea, near, far, edge_east, edge_west)
        far, near = exchanged(near, far)
        if index == STEPS - 1:
            moved, partial = plain_step(moved, energy, wind, sea, west, east)
        else:
            moved, partial, edge_east, edge_west = step(moved, energy, wind, sea, west, east)
    west, east, energy = call(last_edge_kernel, [VMEM] * 3, [column, column, plane])(partial, near, far)
    block = jax.ShapeDtypeStruct((count, bands // count, lanes), F32)
    spectrum_next, local = call(last_kernel, [VMEM] * 7, [full, block], [factors] + staging, [HBM, VMEM])(
        moved, energy, wind, sea, west, east, band_rows.reshape(1, bands)
    )
    spread = lax.all_to_all(local, "gx", 0, 0)
    ocean = call(ocean_kernel, [VMEM], jax.ShapeDtypeStruct((4, bands // count, count * rows), F32), (), VMEM)(spread)
    return (spectrum_next, ocean)


def solution(mesh):
    placed = (
        P(None, None, ("member", "gx"), None),
        P(None, ("member", "gx"), None),
        P("gx", None),
        P(),
    )
    return jax.shard_map(
        per_device,
        mesh=mesh,
        in_specs=placed,
        out_specs=(P(None, None, ("member", "gx"), None), P(None, "gx", "member")),
        check_vma=False,
    )
```
